32 devices in a mesh: grp: 4 (over x, core), dev: 8 (over z, y).
Axes of the slice: x: 2, y: 2, z: 4, core: 2. Of those that a mesh axis runs over, the one named last changes fastest.
Arguments:
- fields: float32 [24, 64, 128, 128], P(None, ('grp', 'dev')), may hold values from -6 to 6
- mix_matrix: float32 [24, 24], replicated, may hold values from -1.25 to 1.25
- laplace_matrix: float32 [24, 24], replicated, may hold values from -0.21875 to 0.21875
Outputs:
- rhs: float32 [24, 64, 128, 128], P(None, ('grp', 'dev'))
- weyl: float32 [2, 64, 128, 128], P(None, 'grp', 'dev')
The draws below stay inside these ranges and needn't reach their ends.
All inputs are finite; a program needn't handle non-finite values.
Results may differ from the reference program's by a relative error of at most 0.0003.
Values sent between devices are 32-bit elements; how exact they have to be, the bound alone decides.
A program may use at most 192 MiB of HBM per device.

```python
import jax
import jax.numpy as jnp
from jax import lax

FIELDS = 24
CZ = 2
NY = 128
NX = 128
NZ = 64


def block_scale(key, dims, split, smallest, top_value):
    level = 1.0
    for position, blocks in split:
        draws = jax.random.uniform(jax.random.fold_in(jax.random.fold_in(key, 6), position), (blocks,), jnp.float32, smallest / len(split), top_value / len(split))
        level = level * jnp.repeat(jnp.exp(draws), dims[position] // blocks).reshape((-1,) + (1,) * (len(dims) - 1 - position))
    return level


def normal_values(stream_key, shape, scale, reach, split=(), kind=jnp.bfloat16):
    values = scale * jax.random.normal(stream_key, shape, jnp.float32)
    if split:
        values = values * block_scale(stream_key, shape, split, -0.22, 0.18)
    return jnp.clip(values, -reach, reach).astype(kind)


def setup_inputs(seed: int = 0) -> dict:
    keys = jax.random.split(jax.random.key(seed), 4)
    fields = normal_values(keys[0], (FIELDS, NZ, NY, NX), 1.0, 6.0, ((1, 32),), jnp.float32)
    mix_matrix = normal_values(keys[1], (FIELDS, FIELDS), FIELDS ** -0.5, 1.25, (), jnp.float32)
    laplace_matrix = normal_values(keys[2], (FIELDS, FIELDS), (FIELDS * 30) ** -0.5, 0.21875, (), jnp.float32)
    return {"fields": fields, "mix_matrix": mix_matrix, "laplace_matrix": laplace_matrix}


def pad_periodic(field, dimension):
    length = field.shape[dimension]
    before = lax.slice_in_dim(field, length - 2, length, axis=dimension)
    after = lax.slice_in_dim(field, 0, 2, axis=dimension)
    return jnp.concatenate([before, field, after], axis=dimension)

def interior(padded, keep):
    result = padded
    for dimension in (1, 2, 3):
        if dimension != keep:
            result = lax.slice_in_dim(result, 2, result.shape[dimension] - 2, axis=dimension)
    return result

def stencil_values(padded, dimension):
    centre = interior(padded, dimension)
    length = centre.shape[dimension] - 4
    return [lax.slice_in_dim(centre, offset, offset + length, axis=dimension) for offset in range(5)]

def first_diff(padded, dimension):
    values = stencil_values(padded, dimension)
    return (values[0] - 8.0 * values[1] + 8.0 * values[3] - values[4]) / 12.0

def second_diff(padded, dimension):
    values = stencil_values(padded, dimension)
    return (-values[0] + 16.0 * values[1] - 30.0 * values[2] + 16.0 * values[3] - values[4]) / 12.0

def laplacian(padded):
    return second_diff(padded, 1) + second_diff(padded, 2) + second_diff(padded, 3)

def evolution(padded, mix_matrix, laplace_matrix):
    centre = interior(padded, 0)
    laplace = laplacian(padded)
    result = jnp.einsum('fg,gzyx->fzyx', mix_matrix, centre, precision=lax.Precision.HIGHEST)
    result = result + jnp.einsum('fg,gzyx->fzyx', laplace_matrix, laplace, precision=lax.Precision.HIGHEST)
    for dimension in (1, 2, 3):
        result = result + centre[11 + dimension][None] * first_diff(padded, dimension)
    return result

def contract(tensor, left, right):
    total = 0.0
    for first in range(3):
        for second in range(3):
            total = total + tensor[first][second] * left[first] * right[second]
    return total

def weyl_scalar(padded, zpos, ypos, xpos):
    table = ((0, 1, 2), (1, 3, 4), (2, 4, 5))
    metric = padded[0:6]
    curv_padded = padded[6:12]
    lap_metric = laplacian(metric)
    curvature = interior(curv_padded, 0)
    gradient = [first_diff(curv_padded, 3 - index) for index in range(3)]
    trace = curvature[0] + curvature[3] + curvature[5]
    electric = []
    curl = []
    for first in range(3):
        erow = []
        crow = []
        for second in range(3):
            value = -0.5 * lap_metric[table[first][second]] - trace * curvature[table[first][second]]
            for middle in range(3):
                value = value + curvature[table[first][middle]] * curvature[table[middle][second]]
            erow.append(value)
            next_one = (first + 1) % 3
            next_two = (first + 2) % 3
            crow.append(gradient[next_one][table[next_two][second]] - gradient[next_two][table[next_one][second]])
        electric.append(erow)
        curl.append(crow)
    magnetic = [[0.5 * (curl[first][second] + curl[second][first]) for second in range(3)] for first in range(3)]
    along_x = xpos[None, None, :]
    along_y = ypos[None, :, None]
    along_z = zpos[:, None, None]
    cylinder = jnp.sqrt(along_x * along_x + along_y * along_y)
    radius = jnp.sqrt(cylinder * cylinder + along_z * along_z)
    theta_vec = (along_z * along_x / (radius * cylinder), along_z * along_y / (radius * cylinder), -cylinder / radius)
    phi_vec = (-along_y / cylinder, along_x / cylinder, 0.0)
    real_part = 0.5 * (contract(electric, theta_vec, theta_vec) - contract(electric, phi_vec, phi_vec)) - contract(magnetic, theta_vec, phi_vec)
    imag_part = -contract(electric, theta_vec, phi_vec) - 0.5 * (contract(magnetic, theta_vec, theta_vec) - contract(magnetic, phi_vec, phi_vec))
    shape = curvature.shape[1:]
    return jnp.stack([jnp.broadcast_to(real_part, shape), jnp.broadcast_to(imag_part, shape)])

def centred(index, count):
    return index.astype(jnp.float32) + 0.5 - 0.5 * count

def reference(fields, mix_matrix, laplace_matrix):
    rows = fields.shape[2]
    width = fields.shape[3]
    padded = pad_periodic(pad_periodic(pad_periodic(fields, 1), 2), 3)
    ypos = centred(jnp.arange(rows, dtype=jnp.int32), rows)
    xpos = centred(jnp.arange(width, dtype=jnp.int32), width)

    def block(index):
        start = (index * CZ).astype(jnp.int32)
        window = lax.dynamic_slice_in_dim(padded, start, CZ + 4, axis=1)
        zpos = centred(start + jnp.arange(CZ, dtype=jnp.int32), NZ)
        return (evolution(window, mix_matrix, laplace_matrix), weyl_scalar(window[0:12], zpos, ypos, xpos))
    rhs_blocks, weyl_blocks = lax.map(block, jnp.arange(NZ // CZ, dtype=jnp.int32))
    rhs = jnp.transpose(rhs_blocks, (1, 0, 2, 3, 4)).reshape(FIELDS, NZ, rows, width)
    weyl = jnp.transpose(weyl_blocks, (1, 0, 2, 3, 4)).reshape(2, NZ, rows, width)
    return (rhs, weyl)
```

```python
import functools

import jax
import jax.numpy as jnp
from jax import lax
from jax.experimental import pallas as pl
from jax.experimental.pallas import tpu as pltpu
from jax.sharding import PartitionSpec as P

AHEAD = 12
LAG = 3
TABLE = ((0, 1, 2), (1, 3, 4), (2, 4, 5))
PAIRS = ((0, 0), (0, 1), (0, 2), (1, 1), (1, 2), (2, 2))


def contract(tensor, left, right):
    total = None
    for first in range(3):
        for second in range(3):
            if left[first] is None or right[second] is None:
                continue
            term = tensor[TABLE[first][second]] * (left[first] * right[second])
            total = term if total is None else total + term
    return total


def weyl_pair(curv, lap, grad, along_x, along_y, along_z):
    trace = curv[0] + curv[3] + curv[5]
    electric = []
    for first, second in PAIRS:
        spot = TABLE[first][second]
        value = -0.5 * lap[spot] - trace * curv[spot]
        for middle in range(3):
            value = value + curv[TABLE[first][middle]] * curv[TABLE[middle][second]]
        electric.append(value)

    def curl(first, second):
        one = (first + 1) % 3
        two = (first + 2) % 3
        return grad[one][TABLE[two][second]] - grad[two][TABLE[one][second]]

    magnetic = [0.5 * (curl(first, second) + curl(second, first)) for first, second in PAIRS]
    square = along_x * along_x + along_y * along_y
    cylinder = jnp.sqrt(square)
    radius = jnp.sqrt(square + along_z * along_z)
    over_cyl = 1.0 / cylinder
    over_rad = 1.0 / radius
    slope = along_z * over_rad * over_cyl
    theta = (slope * along_x, slope * along_y, -cylinder * over_rad)
    phi = (-along_y * over_cyl, along_x * over_cyl, None)
    real = 0.5 * (contract(electric, theta, theta) - contract(electric, phi, phi)) - contract(
        magnetic, theta, phi
    )
    imag = -contract(electric, theta, phi) - 0.5 * (
        contract(magnetic, theta, theta) - contract(magnetic, phi, phi)
    )
    return real, imag


def kernel(
    groups,
    members,
    fields_ref,
    mix_ref,
    lap_ref,
    rhs_ref,
    weyl_ref,
    own,
    halo,
    lapbuf,
    laph,
    gradk,
    wtmp,
    wloc,
    wrecv,
    own_sem,
    send_p,
    recv_p,
    send_r,
    recv_r,
    send_w,
    recv_w,
):
    count, depth, rows, width = own.shape
    slabs = groups * members
    grp = lax.axis_index("grp")
    dev = lax.axis_index("dev")
    slab = grp * members + dev
    side = lax.rem(slab, 2)
    partner = slab + 1 - 2 * side
    follow = lax.rem(slab + slabs + 2 - 4 * side, slabs)
    other = lax.rem(slab + slabs - 2 + 4 * side, slabs)
    per = rows // members

    def place(index):
        return (index // members, lax.rem(index, members))

    load = pltpu.make_async_copy(fields_ref, own, own_sem)
    load.start()

    def peer(offset):
        return lax.rem(dev + offset, members)

    barrier = pltpu.get_barrier_semaphore()
    for target in (follow, other):
        pl.semaphore_signal(
            barrier, inc=1, device_id=place(target), device_id_type=pl.DeviceIdType.MESH
        )
    for offset in range(1, members):
        pl.semaphore_signal(
            barrier, inc=1, device_id=(grp, peer(offset)), device_id_type=pl.DeviceIdType.MESH
        )
    pl.semaphore_wait(barrier, members + 1)

    def exchange(i, slot):
        return pltpu.make_async_remote_copy(
            src_ref=fields_ref.at[i],
            dst_ref=halo.at[slot, i],
            send_sem=send_p.at[i],
            recv_sem=recv_p.at[i],
            device_id=place(partner),
            device_id_type=pl.DeviceIdType.MESH,
        )

    def relay(i, slot):
        return pltpu.make_async_remote_copy(
            src_ref=halo.at[1 - side, i],
            dst_ref=halo.at[slot, i],
            send_sem=send_r.at[i],
            recv_sem=recv_r.at[i],
            device_id=place(follow),
            device_id_type=pl.DeviceIdType.MESH,
        )

    def spread(target, source):
        return pltpu.make_async_remote_copy(
            src_ref=wloc.at[target],
            dst_ref=wrecv.at[source],
            send_sem=send_w.at[target],
            recv_sem=recv_w.at[source],
            device_id=(grp, target),
            device_id_type=pl.DeviceIdType.MESH,
        )

    ahead = min(AHEAD, count)

    @pl.loop(0, ahead)
    def _(i):
        exchange(i, side).start()

    rhs_ref[...] = jnp.zeros_like(rhs_ref)
    load.wait()

    def advance(i):
        exchange(i, 1 - side).wait_recv()
        relay(i, side).start()

        @pl.when(i + ahead < count)
        def _():
            exchange(i + ahead, side).start()

    @pl.loop(0, LAG)
    def _(i):
        advance(i)

    def weyl_local():
        tiles = rows // 8

        @pl.loop(0, depth * tiles)
        def _(t):
            p = t // tiles
            start = pl.multiple_of(lax.rem(t, tiles) * 8, 8)
            strip = pl.ds(start, 8)
            curv = [own[6 + n, p, strip, :] for n in range(6)]
            lap = [laph[n, p, strip, :] for n in range(6)]
            grad = [[gradk[n, a, p, strip, :] for n in range(6)] for a in range(3)]
            lane = lax.broadcasted_iota(jnp.int32, (8, width), 1)
            row = lax.broadcasted_iota(jnp.int32, (8, width), 0) + start
            layer = jnp.full((8, width), slab * depth + p, jnp.int32)
            along_x = lane.astype(jnp.float32) + (0.5 - 0.5 * width)
            along_y = row.astype(jnp.float32) + (0.5 - 0.5 * rows)
            along_z = layer.astype(jnp.float32) + (0.5 - 0.5 * depth * slabs)
            real, imag = weyl_pair(curv, lap, grad, along_x, along_y, along_z)
            wtmp[0, p, strip, :] = real
            wtmp[1, p, strip, :] = imag

        for m in range(members):
            wloc[m] = wtmp[:, :, m * per : (m + 1) * per, :]

    def process(g):
        for p in range(depth):
            f = own[g, p]
            planes = [halo[0, g, 0], halo[0, g, 1], own[g, 0], own[g, 1], halo[1, g, 0], halo[1, g, 1]]
            zm2, zm1, _, zp1, zp2 = planes[p : p + 5]
            ym1, ym2 = pltpu.roll(f, 1, 0), pltpu.roll(f, 2, 0)
            yp1, yp2 = pltpu.roll(f, rows - 1, 0), pltpu.roll(f, rows - 2, 0)
            xm1, xm2 = pltpu.roll(f, 1, 1), pltpu.roll(f, 2, 1)
            xp1, xp2 = pltpu.roll(f, width - 1, 1), pltpu.roll(f, width - 2, 1)
            near = ((zm1 + zp1) + (ym1 + yp1)) + (xm1 + xp1)
            far = ((zm2 + zp2) + (ym2 + yp2)) + (xm2 + xp2)
            lap = (16.0 * near - far - 90.0 * f) * (1.0 / 12.0)
            lapbuf[p] = lap
            gz = (8.0 * (zp1 - zm1) - (zp2 - zm2)) * (1.0 / 12.0)
            gy = (8.0 * (yp1 - ym1) - (yp2 - ym2)) * (1.0 / 12.0)
            gx = (8.0 * (xp1 - xm1) - (xp2 - xm2)) * (1.0 / 12.0)
            rhs_ref[g, p] += own[12, p] * gz + own[13, p] * gy + own[14, p] * gx

            @pl.when(g < 6)
            def _():
                laph[g, p] = lap

            @pl.when(jnp.logical_and(g >= 6, g < 12))
            def _():
                gradk[g - 6, 0, p] = gx
                gradk[g - 6, 1, p] = gy
                gradk[g - 6, 2, p] = gz

        step = 32

        @pl.loop(0, depth * (rows // step))
        def _(t):
            p = t // (rows // step)
            strip = pl.ds(pl.multiple_of(lax.rem(t, rows // step) * step, step), step)
            f = own[g, p, strip, :]
            lap = lapbuf[p, strip, :]
            for c in range(count):
                rhs_ref[c, p, strip, :] += mix_ref[c, g] * f + lap_ref[c, g] * lap

    @pl.loop(0, count)
    def _(g):
        @pl.when(g + LAG < count)
        def _():
            advance(g + LAG)

        relay(g, side).wait_recv()
        process(g)

        @pl.when(g == 11)
        def _():
            weyl_local()

        @pl.when(g == 13)
        def _():
            for offset in range(1, members):
                spread(peer(offset), dev).start()

    def put(source, block):
        for comp in range(2):
            for p in range(depth):
                weyl_ref[comp, source * depth + p] = block[comp, p]

    put(dev, wloc.at[dev])
    for offset in range(1, members):
        source = peer(offset)
        spread(source, source).wait_recv()
        put(source, wrecv.at[source])
    for offset in range(1, members):
        spread(peer(offset), dev).wait_send()

    @pl.loop(0, count)
    def _(i):
        exchange(i, side).wait_send()
        relay(i, side).wait_send()


def per_device(groups, members, fields, mix_matrix, laplace_matrix):
    count, depth, rows, width = fields.shape
    assert depth == 2 and (groups * members) % 2 == 0 and members % 2 == 0
    plane = (rows, width)
    per = rows // members
    vmem = functools.partial(pltpu.VMEM, dtype=jnp.float32)
    dma = pltpu.SemaphoreType.DMA
    return pl.pallas_call(
        functools.partial(kernel, groups, members),
        out_shape=(
            jax.ShapeDtypeStruct(fields.shape, jnp.float32),
            jax.ShapeDtypeStruct((2, depth * members, per, width), jnp.float32),
        ),
        in_specs=[
            pl.BlockSpec(memory_space=pl.ANY),
            pl.BlockSpec(memory_space=pltpu.SMEM),
            pl.BlockSpec(memory_space=pltpu.SMEM),
        ],
        out_specs=(
            pl.BlockSpec(memory_space=pltpu.VMEM),
            pl.BlockSpec(memory_space=pltpu.VMEM),
        ),
        scratch_shapes=[
            vmem((count, depth) + plane),
            vmem((2, count, depth) + plane),
            vmem((depth,) + plane),
            vmem((6, depth) + plane),
            vmem((6, 3, depth) + plane),
            vmem((2, depth) + plane),
            vmem((members, 2, depth, per, width)),
            vmem((members, 2, depth, per, width)),
            dma,
            dma((count,)),
            dma((count,)),
            dma((count,)),
            dma((count,)),
            dma((members,)),
            dma((members,)),
        ],
        compiler_params=pltpu.CompilerParams(
            collective_id=0, has_side_effects=True, vmem_limit_bytes=48 * 1024 * 1024
        ),
        name="evolve",
    )(fields, mix_matrix, laplace_matrix)


def solution(mesh):
    groups, members = mesh.shape["grp"], mesh.shape["dev"]
    return jax.shard_map(
        functools.partial(per_device, groups, members),
        mesh=mesh,
        in_specs=(P(None, ("grp", "dev"), None, None), P(), P()),
        out_specs=(P(None, ("grp", "dev"), None, None), P(None, "grp", "dev", None)),
        check_vma=False,
    )
```

```python
import functools

import jax
import jax.numpy as jnp
from jax import lax
from jax.experimental import pallas as pl
from jax.experimental.pallas import tpu as pltpu
from jax.sharding import PartitionSpec as P

AHEAD = 24
LAG = 4
WEYL_STEPS = 4
TABLE = ((0, 1, 2), (1, 3, 4), (2, 4, 5))
PAIRS = ((0, 0), (0, 1), (0, 2), (1, 1), (1, 2), (2, 2))


def contract(tensor, left, right):
    total = None
    for first in range(3):
        for second in range(3):
            if left[first] is None or right[second] is None:
                continue
            term = tensor[TABLE[first][second]] * (left[first] * right[second])
            total = term if total is None else total + term
    return total


def weyl_pair(curv, lap, grad, along_x, along_y, along_z):
    trace = curv[0] + curv[3] + curv[5]
    electric = []
    for first, second in PAIRS:
        spot = TABLE[first][second]
        value = -0.5 * lap[spot] - trace * curv[spot]
        for middle in range(3):
            value = value + curv[TABLE[first][middle]] * curv[TABLE[middle][second]]
        electric.append(value)

    def curl(first, second):
        one = (first + 1) % 3
        two = (first + 2) % 3
        return grad[one][TABLE[two][second]] - grad[two][TABLE[one][second]]

    magnetic = [0.5 * (curl(first, second) + curl(second, first)) for first, second in PAIRS]
    square = along_x * along_x + along_y * along_y
    cylinder = jnp.sqrt(square)
    radius = jnp.sqrt(square + along_z * along_z)
    over_cyl = 1.0 / cylinder
    over_rad = 1.0 / radius
    slope = along_z * over_rad * over_cyl
    theta = (slope * along_x, slope * along_y, -cylinder * over_rad)
    phi = (-along_y * over_cyl, along_x * over_cyl, None)
    real = 0.5 * (contract(electric, theta, theta) - contract(electric, phi, phi)) - contract(
        magnetic, theta, phi
    )
    imag = -contract(electric, theta, phi) - 0.5 * (
        contract(magnetic, theta, theta) - contract(magnetic, phi, phi)
    )
    return real, imag


def kernel(
    groups,
    members,
    fields_ref,
    mix_hbm,
    lap_hbm,
    rhs_ref,
    weyl_ref,
    own,
    halo,
    lapbuf,
    laph,
    gradk,
    wtmp,
    wloc,
    wrecv,
    mix_ref,
    lap_ref,
    own_sem,
    mat_sem,
    send_p,
    recv_p,
    send_r,
    recv_r,
    send_w,
    recv_w,
):
    count, depth, rows, width = own.shape
    slabs = groups * members
    grp = lax.axis_index("grp")
    dev = lax.axis_index("dev")
    slab = grp * members + dev
    side = lax.rem(slab, 2)
    partner = slab + 1 - 2 * side
    follow = lax.rem(slab + slabs + 2 - 4 * side, slabs)
    other = lax.rem(slab + slabs - 2 + 4 * side, slabs)
    per = rows // members

    def place(index):
        return (index // members, lax.rem(index, members))

    load = pltpu.make_async_copy(fields_ref, own, own_sem)
    load.start()
    small = (
        pltpu.make_async_copy(mix_hbm, mix_ref, mat_sem.at[0]),
        pltpu.make_async_copy(lap_hbm, lap_ref, mat_sem.at[1]),
    )
    for copy in small:
        copy.start()

    def peer(offset):
        return lax.rem(dev + offset, members)

    barrier = pltpu.get_barrier_semaphore()
    for target in (follow, other):
        pl.semaphore_signal(
            barrier, inc=1, device_id=place(target), device_id_type=pl.DeviceIdType.MESH
        )
    for offset in range(1, members):
        pl.semaphore_signal(
            barrier, inc=1, device_id=(grp, peer(offset)), device_id_type=pl.DeviceIdType.MESH
        )
    pl.semaphore_wait(barrier, members + 1)

    def exchange(i, slot):
        return pltpu.make_async_remote_copy(
            src_ref=fields_ref.at[i // depth, lax.rem(i, depth)],
            dst_ref=halo.at[slot, i // depth, lax.rem(i, depth)],
            send_sem=send_p.at[i],
            recv_sem=recv_p.at[i],
            device_id=place(partner),
            device_id_type=pl.DeviceIdType.MESH,
        )

    def relay(i, slot):
        return pltpu.make_async_remote_copy(
            src_ref=halo.at[1 - side, i // depth, lax.rem(i, depth)],
            dst_ref=halo.at[slot, i // depth, lax.rem(i, depth)],
            send_sem=send_r.at[i],
            recv_sem=recv_r.at[i],
            device_id=place(follow),
            device_id_type=pl.DeviceIdType.MESH,
        )

    def spread(target, source):
        return pltpu.make_async_remote_copy(
            src_ref=wloc.at[target],
            dst_ref=wrecv.at[source],
            send_sem=send_w.at[target],
            recv_sem=recv_w.at[source],
            device_id=(grp, target),
            device_id_type=pl.DeviceIdType.MESH,
        )

    chunks = count * depth
    ahead = min(AHEAD, chunks)

    @pl.loop(0, ahead)
    def _(i):
        exchange(i, side).start()

    rhs_ref[...] = jnp.zeros_like(rhs_ref)
    load.wait()
    for copy in small:
        copy.wait()

    def advance(i):
        exchange(i, 1 - side).wait_recv()
        relay(i, side).start()

        @pl.when(i + ahead < chunks)
        def _():
            exchange(i + ahead, side).start()

    @pl.loop(0, LAG * depth)
    def _(i):
        advance(i)

    def weyl_local(part):
        tiles = rows // 8
        share = depth * tiles // WEYL_STEPS

        @pl.loop(0, share)
        def _(u):
            t = part * share + u
            p = t // tiles
            start = pl.multiple_of(lax.rem(t, tiles) * 8, 8)
            strip = pl.ds(start, 8)
            curv = [own[6 + n, p, strip, :] for n in range(6)]
            lap = [laph[n, p, strip, :] for n in range(6)]
            grad = [[gradk[n, a, p, strip, :] for n in range(6)] for a in range(3)]
            lane = lax.broadcasted_iota(jnp.int32, (8, width), 1)
            row = lax.broadcasted_iota(jnp.int32, (8, width), 0) + start
            layer = jnp.full((8, width), slab * depth + p, jnp.int32)
            along_x = lane.astype(jnp.float32) + (0.5 - 0.5 * width)
            along_y = row.astype(jnp.float32) + (0.5 - 0.5 * rows)
            along_z = layer.astype(jnp.float32) + (0.5 - 0.5 * depth * slabs)
            real, imag = weyl_pair(curv, lap, grad, along_x, along_y, along_z)
            wtmp[0, p, strip, :] = real
            wtmp[1, p, strip, :] = imag

    def process(g):
        for p in range(depth):
            f = own[g, p]
            planes = [halo[0, g, 0], halo[0, g, 1], own[g, 0], own[g, 1], halo[1, g, 0], halo[1, g, 1]]
            zm2, zm1, _, zp1, zp2 = planes[p : p + 5]
            ym1, ym2 = pltpu.roll(f, 1, 0), pltpu.roll(f, 2, 0)
            yp1, yp2 = pltpu.roll(f, rows - 1, 0), pltpu.roll(f, rows - 2, 0)
            xm1, xm2 = pltpu.roll(f, 1, 1), pltpu.roll(f, 2, 1)
            xp1, xp2 = pltpu.roll(f, width - 1, 1), pltpu.roll(f, width - 2, 1)
            near = ((zm1 + zp1) + (ym1 + yp1)) + (xm1 + xp1)
            far = ((zm2 + zp2) + (ym2 + yp2)) + (xm2 + xp2)
            lap = (16.0 * near - far - 90.0 * f) * (1.0 / 12.0)
            lapbuf[p] = lap
            gz = (8.0 * (zp1 - zm1) - (zp2 - zm2)) * (1.0 / 12.0)
            gy = (8.0 * (yp1 - ym1) - (yp2 - ym2)) * (1.0 / 12.0)
            gx = (8.0 * (xp1 - xm1) - (xp2 - xm2)) * (1.0 / 12.0)
            rhs_ref[g, p] += own[12, p] * gz + own[13, p] * gy + own[14, p] * gx

            @pl.when(g < 6)
            def _():
                laph[g, p] = lap

            @pl.when(jnp.logical_and(g >= 6, g < 12))
            def _():
                gradk[g - 6, 0, p] = gx
                gradk[g - 6, 1, p] = gy
                gradk[g - 6, 2, p] = gz

        step = 32

        @pl.loop(0, depth * (rows // step))
        def _(t):
            p = t // (rows // step)
            strip = pl.ds(pl.multiple_of(lax.rem(t, rows // step) * step, step), step)
            f = own[g, p, strip, :]
            lap = lapbuf[p, strip, :]
            for c in range(count):
                rhs_ref[c, p, strip, :] += mix_ref[c, g] * f + lap_ref[c, g] * lap

    @pl.loop(0, count)
    def _(g):
        @pl.when(g + LAG < count)
        def _():
            for p in range(depth):
                advance((g + LAG) * depth + p)

        for p in range(depth):
            relay(g * depth + p, side).wait_recv()
        process(g)

        @pl.when(jnp.logical_and(g >= 11, g < 11 + WEYL_STEPS))
        def _():
            weyl_local(g - 11)

        @pl.when(g == 11 + WEYL_STEPS)
        def _():
            for m in range(members):
                wloc[m] = wtmp[:, :, m * per : (m + 1) * per, :]

        @pl.when(g == 12 + WEYL_STEPS)
        def _():
            for offset in range(1, members):
                spread(peer(offset), dev).start()

    def put(source, block):
        for comp in range(2):
            for p in range(depth):
                weyl_ref[comp, source * depth + p] = block[comp, p]

    put(dev, wloc.at[dev])
    for offset in range(1, members):
        source = peer(offset)
        spread(source, source).wait_recv()
        put(source, wrecv.at[source])
    for offset in range(1, members):
        spread(peer(offset), dev).wait_send()

    @pl.loop(0, chunks)
    def _(i):
        exchange(i, side).wait_send()
        relay(i, side).wait_send()


def per_device(groups, members, fields, mix_matrix, laplace_matrix):
    count, depth, rows, width = fields.shape
    assert depth == 2 and (groups * members) % 2 == 0 and members % 2 == 0
    plane = (rows, width)
    per = rows // members
    vmem = functools.partial(pltpu.VMEM, dtype=jnp.float32)
    dma = pltpu.SemaphoreType.DMA
    return pl.pallas_call(
        functools.partial(kernel, groups, members),
        out_shape=(
            jax.ShapeDtypeStruct(fields.shape, jnp.float32),
            jax.ShapeDtypeStruct((2, depth * members, per, width), jnp.float32),
        ),
        in_specs=[
            pl.BlockSpec(memory_space=pltpu.HBM),
            pl.BlockSpec(memory_space=pltpu.HBM),
            pl.BlockSpec(memory_space=pltpu.HBM),
        ],
        out_specs=(
            pl.BlockSpec(memory_space=pltpu.VMEM),
            pl.BlockSpec(memory_space=pltpu.VMEM),
        ),
        scratch_shapes=[
            vmem((count, depth) + plane),
            vmem((2, count, depth) + plane),
            vmem((depth,) + plane),
            vmem((6, depth) + plane),
            vmem((6, 3, depth) + plane),
            vmem((2, depth) + plane),
            vmem((members, 2, depth, per, width)),
            vmem((members, 2, depth, per, width)),
            pltpu.SMEM((count, count), jnp.float32),
            pltpu.SMEM((count, count), jnp.float32),
            dma,
            dma((2,)),
            dma((count * depth,)),
            dma((count * depth,)),
            dma((count * depth,)),
            dma((count * depth,)),
            dma((members,)),
            dma((members,)),
        ],
        compiler_params=pltpu.CompilerParams(
            collective_id=0, has_side_effects=True, vmem_limit_bytes=48 * 1024 * 1024
        ),
        name="evolve",
    )(fields, mix_matrix, laplace_matrix)


def solution(mesh):
    groups, members = mesh.shape["grp"], mesh.shape["dev"]
    return jax.shard_map(
        functools.partial(per_device, groups, members),
        mesh=mesh,
        in_specs=(P(None, ("grp", "dev"), None, None), P(), P()),
        out_specs=(P(None, ("grp", "dev"), None, None), P(None, "grp", "dev", None)),
        check_vma=False,
    )
```

```python
import functools

import jax
import jax.numpy as jnp
from jax import lax
from jax.experimental import pallas as pl
from jax.experimental.pallas import tpu as pltpu
from jax.sharding import PartitionSpec as P

AHEAD = 24
LAG = 4
WEYL_STEPS = 4
TABLE = ((0, 1, 2), (1, 3, 4), (2, 4, 5))
PAIRS = ((0, 0), (0, 1), (0, 2), (1, 1), (1, 2), (2, 2))


def contract(tensor, left, right):
    total = None
    for first in range(3):
        for second in range(3):
            if left[first] is None or right[second] is None:
                continue
            term = tensor[TABLE[first][second]] * (left[first] * right[second])
            total = term if total is None else total + term
    return total


def weyl_pair(curv, lap, grad, along_x, along_y, along_z):
    trace = curv[0] + curv[3] + curv[5]
    electric = []
    for first, second in PAIRS:
        spot = TABLE[first][second]
        value = -0.5 * lap[spot] - trace * curv[spot]
        for middle in range(3):
            value = value + curv[TABLE[first][middle]] * curv[TABLE[middle][second]]
        electric.append(value)

    def curl(first, second):
        one = (first + 1) % 3
        two = (first + 2) % 3
        return grad[one][TABLE[two][second]] - grad[two][TABLE[one][second]]

    magnetic = [0.5 * (curl(first, second) + curl(second, first)) for first, second in PAIRS]
    square = along_x * along_x + along_y * along_y
    cylinder = jnp.sqrt(square)
    radius = jnp.sqrt(square + along_z * along_z)
    over_cyl = 1.0 / cylinder
    over_rad = 1.0 / radius
    slope = along_z * over_rad * over_cyl
    theta = (slope * along_x, slope * along_y, -cylinder * over_rad)
    phi = (-along_y * over_cyl, along_x * over_cyl, None)
    real = 0.5 * (contract(electric, theta, theta) - contract(electric, phi, phi)) - contract(
        magnetic, theta, phi
    )
    imag = -contract(electric, theta, phi) - 0.5 * (
        contract(magnetic, theta, theta) - contract(magnetic, phi, phi)
    )
    return real, imag


def kernel(
    groups,
    members,
    fields_ref,
    mix_hbm,
    lap_hbm,
    rhs_ref,
    weyl_ref,
    own,
    halo,
    lapbuf,
    laph,
    gradk,
    wtmp,
    wloc,
    wrecv,
    mix_ref,
    lap_ref,
    own_sem,
    mat_sem,
    send_p,
    recv_p,
    send_r,
    recv_r,
    send_w,
    recv_w,
):
    count, depth, rows, width = own.shape
    slabs = groups * members
    grp = lax.axis_index("grp")
    dev = lax.axis_index("dev")
    slab = grp * members + dev
    side = lax.rem(slab, 2)
    partner = slab + 1 - 2 * side
    follow = lax.rem(slab + slabs + 2 - 4 * side, slabs)
    other = lax.rem(slab + slabs - 2 + 4 * side, slabs)
    per = rows // members

    def place(index):
        return (index // members, lax.rem(index, members))

    load = pltpu.make_async_copy(fields_ref, own, own_sem)
    load.start()
    small = (
        pltpu.make_async_copy(mix_hbm, mix_ref, mat_sem.at[0]),
        pltpu.make_async_copy(lap_hbm, lap_ref, mat_sem.at[1]),
    )
    for copy in small:
        copy.start()

    def peer(offset):
        return lax.rem(dev + offset, members)

    barrier = pltpu.get_barrier_semaphore()
    for target in (follow, other):
        pl.semaphore_signal(
            barrier, inc=1, device_id=place(target), device_id_type=pl.DeviceIdType.MESH
        )
    for offset in range(1, members):
        pl.semaphore_signal(
            barrier, inc=1, device_id=(grp, peer(offset)), device_id_type=pl.DeviceIdType.MESH
        )
    pl.semaphore_wait(barrier, members + 1)

    def exchange(i, slot):
        return pltpu.make_async_remote_copy(
            src_ref=fields_ref.at[i // depth, lax.rem(i, depth)],
            dst_ref=halo.at[slot, i // depth, lax.rem(i, depth)],
            send_sem=send_p.at[i],
            recv_sem=recv_p.at[i],
            device_id=place(partner),
            device_id_type=pl.DeviceIdType.MESH,
        )

    def relay(i, slot):
        return pltpu.make_async_remote_copy(
            src_ref=halo.at[1 - side, i // depth, lax.rem(i, depth)],
            dst_ref=halo.at[slot, i // depth, lax.rem(i, depth)],
            send_sem=send_r.at[i],
            recv_sem=recv_r.at[i],
            device_id=place(follow),
            device_id_type=pl.DeviceIdType.MESH,
        )

    def spread(target, source):
        return pltpu.make_async_remote_copy(
            src_ref=wloc.at[target],
            dst_ref=wrecv.at[source],
            send_sem=send_w.at[target],
            recv_sem=recv_w.at[source],
            device_id=(grp, target),
            device_id_type=pl.DeviceIdType.MESH,
        )

    chunks = count * depth
    ahead = min(AHEAD, chunks)

    @pl.loop(0, ahead)
    def _(i):
        exchange(i, side).start()

    rhs_ref[...] = jnp.zeros_like(rhs_ref)
    load.wait()
    for copy in small:
        copy.wait()

    def advance(i):
        exchange(i, 1 - side).wait_recv()
        relay(i, side).start()

        @pl.when(i + ahead < chunks)
        def _():
            exchange(i + ahead, side).start()

    @pl.loop(0, LAG * depth)
    def _(i):
        advance(i)

    def weyl_local(part):
        tiles = rows // 8
        share = depth * tiles // WEYL_STEPS

        @pl.loop(0, share)
        def _(u):
            t = part * share + u
            p = t // tiles
            start = pl.multiple_of(lax.rem(t, tiles) * 8, 8)
            strip = pl.ds(start, 8)
            curv = [own[6 + n, p, strip, :] for n in range(6)]
            lap = [laph[n, p, strip, :] for n in range(6)]
            grad = [[gradk[n, a, p, strip, :] for n in range(6)] for a in range(3)]
            lane = lax.broadcasted_iota(jnp.int32, (8, width), 1)
            row = lax.broadcasted_iota(jnp.int32, (8, width), 0) + start
            layer = jnp.full((8, width), slab * depth + p, jnp.int32)
            along_x = lane.astype(jnp.float32) + (0.5 - 0.5 * width)
            along_y = row.astype(jnp.float32) + (0.5 - 0.5 * rows)
            along_z = layer.astype(jnp.float32) + (0.5 - 0.5 * depth * slabs)
            real, imag = weyl_pair(curv, lap, grad, along_x, along_y, along_z)
            wtmp[0, p, strip, :] = real
            wtmp[1, p, strip, :] = imag

    def process(g):
        for p in range(depth):
            f = own[g, p]
            planes = [halo[0, g, 0], halo[0, g, 1], own[g, 0], own[g, 1], halo[1, g, 0], halo[1, g, 1]]
            zm2, zm1, _, zp1, zp2 = planes[p : p + 5]
            ym1, ym2 = pltpu.roll(f, 1, 0), pltpu.roll(f, 2, 0)
            yp1, yp2 = pltpu.roll(f, rows - 1, 0), pltpu.roll(f, rows - 2, 0)
            xm1, xm2 = pltpu.roll(f, 1, 1), pltpu.roll(f, 2, 1)
            xp1, xp2 = pltpu.roll(f, width - 1, 1), pltpu.roll(f, width - 2, 1)
            near = ((zm1 + zp1) + (ym1 + yp1)) + (xm1 + xp1)
            far = ((zm2 + zp2) + (ym2 + yp2)) + (xm2 + xp2)
            lap = (16.0 * near - far - 90.0 * f) * (1.0 / 12.0)
            lapbuf[p] = lap
            gz = (8.0 * (zp1 - zm1) - (zp2 - zm2)) * (1.0 / 12.0)
            gy = (8.0 * (yp1 - ym1) - (yp2 - ym2)) * (1.0 / 12.0)
            gx = (8.0 * (xp1 - xm1) - (xp2 - xm2)) * (1.0 / 12.0)
            rhs_ref[g, p] += own[12, p] * gz + own[13, p] * gy + own[14, p] * gx

            @pl.when(g < 6)
            def _():
                laph[g, p] = lap

            @pl.when(jnp.logical_and(g >= 6, g < 12))
            def _():
                gradk[g - 6, 0, p] = gx
                gradk[g - 6, 1, p] = gy
                gradk[g - 6, 2, p] = gz

        step = 32

        @pl.loop(0, depth * (rows // step))
        def _(t):
            p = t // (rows // step)
            strip = pl.ds(pl.multiple_of(lax.rem(t, rows // step) * step, step), step)
            f = own[g, p, strip, :]
            lap = lapbuf[p, strip, :]
            for c in range(count):
                rhs_ref[c, p, strip, :] += mix_ref[c, g] * f + lap_ref[c, g] * lap

    @pl.loop(0, count)
    def _(g):
        @pl.when(g + LAG < count)
        def _():
            for p in range(depth):
                advance((g + LAG) * depth + p)

        for p in range(depth):
            relay(g * depth + p, side).wait_recv()
        process(g)

        @pl.when(jnp.logical_and(g >= 11, g < 11 + WEYL_STEPS))
        def _():
            weyl_local(g - 11)

        @pl.when(g == 11 + WEYL_STEPS)
        def _():
            for m in range(members):
                wloc[m] = wtmp[:, :, m * per : (m + 1) * per, :]

        @pl.when(g == count - LAG)
        def _():
            for offset in range(1, members):
                spread(peer(offset), dev).start()

    def put(source, block):
        for comp in range(2):
            for p in range(depth):
                weyl_ref[comp, source * depth + p] = block[comp, p]

    put(dev, wloc.at[dev])
    for offset in range(1, members):
        source = peer(offset)
        spread(source, source).wait_recv()
        put(source, wrecv.at[source])
    for offset in range(1, members):
        spread(peer(offset), dev).wait_send()

    @pl.loop(0, chunks)
    def _(i):
        exchange(i, side).wait_send()
        relay(i, side).wait_send()


def per_device(groups, members, fields, mix_matrix, laplace_matrix):
    count, depth, rows, width = fields.shape
    assert depth == 2 and (groups * members) % 2 == 0 and members % 2 == 0
    plane = (rows, width)
    per = rows // members
    vmem = functools.partial(pltpu.VMEM, dtype=jnp.float32)
    dma = pltpu.SemaphoreType.DMA
    return pl.pallas_call(
        functools.partial(kernel, groups, members),
        out_shape=(
            jax.ShapeDtypeStruct(fields.shape, jnp.float32),
            jax.ShapeDtypeStruct((2, depth * members, per, width), jnp.float32),
        ),
        in_specs=[
            pl.BlockSpec(memory_space=pltpu.HBM),
            pl.BlockSpec(memory_space=pltpu.HBM),
            pl.BlockSpec(memory_space=pltpu.HBM),
        ],
        out_specs=(
            pl.BlockSpec(memory_space=pltpu.VMEM),
            pl.BlockSpec(memory_space=pltpu.VMEM),
        ),
        scratch_shapes=[
            vmem((count, depth) + plane),
            vmem((2, count, depth) + plane),
            vmem((depth,) + plane),
            vmem((6, depth) + plane),
            vmem((6, 3, depth) + plane),
            vmem((2, depth) + plane),
            vmem((members, 2, depth, per, width)),
            vmem((members, 2, depth, per, width)),
            pltpu.SMEM((count, count), jnp.float32),
            pltpu.SMEM((count, count), jnp.float32),
            dma,
            dma((2,)),
            dma((count * depth,)),
            dma((count * depth,)),
            dma((count * depth,)),
            dma((count * depth,)),
            dma((members,)),
            dma((members,)),
        ],
        compiler_params=pltpu.CompilerParams(
            collective_id=0, has_side_effects=True, vmem_limit_bytes=48 * 1024 * 1024
        ),
        name="evolve",
    )(
        fields,
        pltpu.with_memory_space_constraint(mix_matrix, pltpu.HBM),
        pltpu.with_memory_space_constraint(laplace_matrix, pltpu.HBM),
    )


def solution(mesh):
    groups, members = mesh.shape["grp"], mesh.shape["dev"]
    return jax.shard_map(
        functools.partial(per_device, groups, members),
        mesh=mesh,
        in_specs=(P(None, ("grp", "dev"), None, None), P(), P()),
        out_specs=(P(None, ("grp", "dev"), None, None), P(None, "grp", "dev", None)),
        check_vma=False,
    )
```
